32 devices in a mesh: dp: 16 (over z, y, core), tensor: 2 (over x).
Axes of the slice: x: 2, y: 2, z: 4, core: 2. Of those that a mesh axis runs over, the one named last changes fastest.
Arguments:
- expert_act: bfloat16 [16384, 2880], P(('dp', 'tensor')), may hold values from -6 to 6
- grad_out: bfloat16 [32768, 1440], P(('dp', 'tensor')), may hold values from -6 to 6
- slot_token: int32 [16384], P(('dp', 'tensor')), may hold values from 0 to 1023, as said below
- slot_prob: float32 [16384], P(('dp', 'tensor')), may hold values from 0.2 to 1
- live_count: int32 [32], P(('dp', 'tensor')), may hold values from 128 to 512, as said below
Outputs:
- weight_grad: float32 [2880, 1440], P('dp', 'tensor')
The draws below stay inside these ranges and needn't reach their ends.
Inputs may be any that keep to these rules, and one draw needn't show every extreme that they name: `slot_token`: each device's 512 entries are distinct token indices of that device. `live_count`: each entry is 512 // j for some j of 1 to 4.
All inputs are finite; a program needn't handle non-finite values.
Results may differ from the reference program's by a relative error of at most 0.0029.
Values may be sent and summed in bfloat16 or wider, within the bound.
A program may use at most 128 MiB of HBM per device.

```python
import math
import jax
import jax.numpy as jnp
from jax import lax

D = 1440
FF = 2880
CAP = 512
TOK_DEV = 1024
SLOTS = 16384
TOKENS = 32768


def draw_slot_token(key, part):
    device_total = SLOTS // CAP
    device_keys = jax.random.split(jax.random.fold_in(key, 11), device_total)

    def shuffled(seed_key):
        return jax.random.permutation(seed_key, TOK_DEV)[:CAP].astype(jnp.int32)
    return jax.vmap(shuffled)(device_keys).reshape(-1).astype(jnp.int32)


def draw_live_count(key, part):
    device_total = SLOTS // CAP
    first_key = jax.random.fold_in(key, 21)
    second_key = jax.random.fold_in(key, 22)
    divisor = jax.random.randint(first_key, (device_total,), 1, 5)
    counted = (CAP // divisor).astype(jnp.int32)
    fullest = jax.random.randint(second_key, (), 0, device_total)
    return counted.at[fullest].set(CAP).astype(jnp.int32)


def block_levels(key, shape, shards, low, high):
    factor_of = 1.0
    for dim, blocks in shards:
        steps = jax.random.uniform(jax.random.fold_in(jax.random.fold_in(key, 6), dim), (blocks,), jnp.float32, low / len(shards), high / len(shards))
        factor_of = factor_of * jnp.repeat(jnp.exp(steps), shape[dim] // blocks).reshape((-1,) + (1,) * (len(shape) - 1 - dim))
    return factor_of


def normal_values(stream_key, dims, width, reach, pieces=(), kind=jnp.bfloat16):
    entries = jax.random.normal(stream_key, dims, jnp.float32) * width
    if len(pieces) > 0:
        entries = block_levels(stream_key, dims, pieces, -0.22, 0.18) * entries
    return jnp.clip(entries, min=-reach, max=reach).astype(kind)


def setup_inputs(seed: int = 0) -> dict:
    splits = jax.random.split(jax.random.key(seed), 6)
    expert_act = normal_values(splits[0], (SLOTS, FF), 1.0, 6.0, ((0, 32),))
    grad_out = normal_values(splits[1], (TOKENS, D), 1.0, 6.0, ((0, 32),))
    slot_token = draw_slot_token(jax.random.fold_in(splits[5], 71), 0)
    slot_prob = jnp.clip(jnp.exp(math.log(1.0) - 1.609438 * jax.random.uniform(splits[3], (SLOTS,), jnp.float32) ** block_levels(splits[3], (SLOTS,), ((0, 32),), -0.2, 0.2)), 0.2, 1.0)
    live_count = draw_live_count(jax.random.fold_in(splits[5], 71), 0)
    return dict(expert_act=expert_act, grad_out=grad_out, slot_token=slot_token, slot_prob=slot_prob, live_count=live_count)


def reference(expert_act, grad_out, slot_token, slot_prob, live_count):
    slot_total = expert_act.shape[0]
    position = jnp.arange(slot_total, dtype=jnp.int32)
    owner_dev = (position // CAP).astype(jnp.int32)
    token_rows = (slot_token + owner_dev * TOK_DEV).astype(jnp.int32)
    live_mask = position % CAP < live_count[owner_dev]
    weighting = jnp.where(live_mask, slot_prob, jnp.zeros_like(slot_prob))
    picked = grad_out[token_rows].astype(jnp.float32)
    weighted = (picked * weighting[:, None]).astype(jnp.bfloat16)
    gradient = lax.dot_general(expert_act, weighted, (((0,), (0,)), ((), ())), preferred_element_type=jnp.float32)
    return gradient * (1.0 / math.sqrt(slot_total))
```

```python
import functools
import math

import jax
import jax.numpy as jnp
from jax import lax
from jax.experimental import pallas as pl
from jax.experimental.pallas import tpu as pltpu
from jax.sharding import PartitionSpec as P

MESH = pl.DeviceIdType.MESH


def kernel(
    outer,
    acts_ref, grad_ref, token_ref, weight_ref, out_ref,
    peer_acts, mine, peer,
    send_a, recv_a, send_b, recv_b, send_z, recv_z,
    pair_sems, a_sems, b_sems, z_sems,
):
    dp = lax.axis_index("dp")
    half = lax.axis_index("tensor")
    core = lax.rem(dp, 2)
    mid = lax.rem(dp // 2, 2)
    own = dp // 4
    my_a = half * (1 - core) + mid * core
    my_b = mid * (1 - core) + half * core
    flip_mid = dp + 2 - 4 * mid
    pair_dev = {"dp": dp + 1 - 2 * core, "tensor": half}
    a_dev = {
        "dp": dp * (1 - core) + flip_mid * core,
        "tensor": (1 - half) * (1 - core) + half * core,
    }
    b_dev = {
        "dp": flip_mid * (1 - core) + dp * core,
        "tensor": half * (1 - core) + (1 - half) * core,
    }

    def z_dev(step):
        return {"dp": dp + (target(step) - own) * 4, "tensor": half}

    def target(step):
        return lax.rem(own + 1 + step, outer)

    def remote(src, dst, sems, device):
        return pltpu.make_async_remote_copy(
            src_ref=src, dst_ref=dst, send_sem=sems[0], recv_sem=sems[1],
            device_id=device, device_id_type=MESH,
        )

    barrier = pltpu.get_barrier_semaphore()
    for device in [pair_dev, a_dev, b_dev] + [z_dev(s) for s in range(outer - 1)]:
        pl.semaphore_signal(barrier, inc=1, device_id=device, device_id_type=MESH)
    pl.semaphore_wait(barrier, outer + 2)

    acts_copy = remote(
        acts_ref.at[1 - core], peer_acts, (pair_sems.at[0], pair_sems.at[1]), pair_dev
    )
    acts_copy.start()

    slots, tokens = token_ref.shape[0], grad_ref.shape[0]
    width = mine.shape[2]
    chosen = lax.broadcasted_iota(jnp.int32, (slots, tokens), 1) == token_ref[...]
    onehot = jnp.where(chosen, 1.0, 0.0).astype(jnp.bfloat16)
    picked = jnp.dot(onehot, grad_ref[...], preferred_element_type=jnp.float32)
    weighted = (picked * weight_ref[...]).astype(jnp.bfloat16)
    mine[0] = weighted[:, :width]
    mine[1] = weighted[:, width:]
    grad_copy = remote(mine, peer, (pair_sems.at[2], pair_sems.at[3]), pair_dev)
    grad_copy.start()
    acts_copy.wait_recv()
    grad_copy.wait_recv()

    def term(step, a, b):
        row = target(step) * 2 + b * (1 - core) + a * core
        column = a * (1 - core) + b * core
        return jnp.dot(
            acts_ref[core, row], mine[column], preferred_element_type=jnp.float32
        ) + jnp.dot(
            peer_acts[row], peer[column], preferred_element_type=jnp.float32
        )

    def copy_a(step, k):
        return remote(
            send_a.at[step, k], recv_a.at[step, k],
            (a_sems.at[0, step, k], a_sems.at[1, step, k]), a_dev,
        )

    def copy_b(step):
        return remote(
            send_b.at[step], recv_b.at[step],
            (b_sems.at[0, step], b_sems.at[1, step]), b_dev,
        )

    def copy_z(step):
        return remote(
            send_z.at[step], recv_z.at[step],
            (z_sems.at[0, step], z_sems.at[1, step]), z_dev(step),
        )

    def first(step, carry):
        for k in range(2):
            b = 1 - my_b if k == 0 else my_b
            send_a[step, k] = term(step, 1 - my_a, b).astype(jnp.bfloat16)
            copy_a(step, k).start()
        return carry

    def second(step):
        total = term(step, my_a, 1 - my_b)
        copy_a(step, 0).wait_recv()
        total = total + recv_a[step, 0].astype(jnp.float32)
        send_b[step] = total.astype(jnp.bfloat16)
        copy_b(step).start()

    def third(step):
        total = term(step, my_a, my_b)
        copy_a(step, 1).wait_recv()
        total = total + recv_a[step, 1].astype(jnp.float32)
        copy_b(step).wait_recv()
        return total + recv_b[step].astype(jnp.float32)

    def later(step, carry):
        second(step)
        send_z[step - 1] = third(step - 1).astype(jnp.bfloat16)
        copy_z(step - 1).start()
        return carry

    lax.fori_loop(0, outer, first, 0)
    second(0)
    lax.fori_loop(1, outer, later, 0)
    out_ref[...] = third(outer - 1)

    def add(step, carry):
        copy_z(step).wait_recv()
        out_ref[...] += recv_z[step].astype(jnp.float32)
        return carry

    lax.fori_loop(0, outer - 1, add, 0)

    def drain(step, carry):
        copy_a(step, 0).wait_send()
        copy_a(step, 1).wait_send()
        copy_b(step).wait_send()
        return carry

    lax.fori_loop(0, outer, drain, 0)

    def drain_z(step, carry):
        copy_z(step).wait_send()
        return carry

    lax.fori_loop(0, outer - 1, drain_z, 0)
    acts_copy.wait_send()
    grad_copy.wait_send()


def shards(expert_act, grad_out, slot_token, slot_prob, live_count):
    slots, hidden = expert_act.shape
    ranks, halves = lax.axis_size("dp"), lax.axis_size("tensor")
    outer = ranks // 4
    rows, columns = hidden // ranks, grad_out.shape[1] // halves
    scaling = 1.0 / math.sqrt(slots * ranks * halves)
    live = jnp.arange(slots, dtype=jnp.int32) < live_count[0]
    weighting = jnp.where(live, slot_prob, jnp.zeros_like(slot_prob))
    acts = expert_act.T.reshape(outer * 2, 2, rows, slots).transpose(1, 0, 2, 3)
    bf16, dma = jnp.bfloat16, pltpu.SemaphoreType.DMA
    total = pl.pallas_call(
        functools.partial(kernel, outer),
        out_shape=jax.ShapeDtypeStruct((rows, columns), jnp.float32),
        in_specs=[pl.BlockSpec(memory_space=pltpu.VMEM)] * 4,
        out_specs=pl.BlockSpec(memory_space=pltpu.VMEM),
        scratch_shapes=[
            pltpu.VMEM((outer * 2, rows, slots), bf16),
            pltpu.VMEM((2, slots, columns), bf16),
            pltpu.VMEM((2, slots, columns), bf16),
            pltpu.VMEM((outer, 2, rows, columns), bf16),
            pltpu.VMEM((outer, 2, rows, columns), bf16),
            pltpu.VMEM((outer, rows, columns), bf16),
            pltpu.VMEM((outer, rows, columns), bf16),
            pltpu.VMEM((outer - 1, rows, columns), bf16),
            pltpu.VMEM((outer - 1, rows, columns), bf16),
            dma((4,)),
            dma((2, outer, 2)),
            dma((2, outer)),
            dma((2, outer - 1)),
        ],
        compiler_params=pltpu.CompilerParams(
            collective_id=0, has_side_effects=True, vmem_limit_bytes=60 * 2**20
        ),
    )(acts, grad_out, slot_token[:, None], weighting[:, None])
    return total * scaling


def solution(mesh):
    return jax.shard_map(
        shards,
        mesh=mesh,
        in_specs=(
            P(("dp", "tensor"), None),
            P(("dp", "tensor"), None),
            P(("dp", "tensor")),
            P(("dp", "tensor")),
            P(("dp", "tensor")),
        ),
        out_specs=P("dp", "tensor"),
        check_vma=False,
    )
```

```python
import functools
import math

import jax
import jax.numpy as jnp
from jax import lax
from jax.experimental import pallas as pl
from jax.experimental.pallas import tpu as pltpu
from jax.sharding import PartitionSpec as P

MESH = pl.DeviceIdType.MESH


def kernel(
    outer,
    acts_hbm, grad_hbm, token_ref, prob_ref, live_ref, out_ref,
    acts_raw, grad_raw, acts, peer_acts, mine, peer,
    send_a, recv_a, send_b, recv_b, send_z, recv_z,
    load_sems, pair_sems, a_sems, b_sems, z_sems,
):
    dp = lax.axis_index("dp")
    half = lax.axis_index("tensor")
    core = lax.rem(dp, 2)
    mid = lax.rem(dp // 2, 2)
    own = dp // 4
    my_a = half * (1 - core) + mid * core
    my_b = mid * (1 - core) + half * core
    flip_mid = dp + 2 - 4 * mid
    pair_dev = {"dp": dp + 1 - 2 * core, "tensor": half}
    a_dev = {
        "dp": dp * (1 - core) + flip_mid * core,
        "tensor": (1 - half) * (1 - core) + half * core,
    }
    b_dev = {
        "dp": flip_mid * (1 - core) + dp * core,
        "tensor": half * (1 - core) + (1 - half) * core,
    }

    def z_dev(step):
        return {"dp": dp + (target(step) - own) * 4, "tensor": half}

    def target(step):
        return lax.rem(own + 1 + step, outer)

    def remote(src, dst, sems, device):
        return pltpu.make_async_remote_copy(
            src_ref=src, dst_ref=dst, send_sem=sems[0], recv_sem=sems[1],
            device_id=device, device_id_type=MESH,
        )

    load_acts = pltpu.make_async_copy(acts_hbm, acts_raw, load_sems.at[0])
    load_acts.start()
    grad_order = (1 - half, half)
    load_grads = [
        pltpu.make_async_copy(grad_hbm.at[g], grad_raw.at[g], load_sems.at[1 + i])
        for i, g in enumerate(grad_order)
    ]
    for load in load_grads:
        load.start()

    barrier = pltpu.get_barrier_semaphore()
    for device in [pair_dev, a_dev, b_dev] + [z_dev(s) for s in range(outer - 1)]:
        pl.semaphore_signal(barrier, inc=1, device_id=device, device_id_type=MESH)

    slots, tokens = token_ref.shape[1], grad_raw.shape[2]
    chosen = lax.broadcasted_iota(jnp.int32, (tokens, slots), 0) == token_ref[...]
    onehot = jnp.where(chosen, 1.0, 0.0).astype(jnp.bfloat16)
    live = lax.broadcasted_iota(jnp.int32, (1, slots), 1) < live_ref[0]
    weight = jnp.where(live, prob_ref[...], 0.0)

    load_acts.wait()
    rows = acts.shape[2]
    for k in range(outer * 4):
        acts[k % 2, k // 2] = acts_raw[k * rows : (k + 1) * rows, :]
    pl.semaphore_wait(barrier, outer + 2)
    acts_copy = remote(
        acts.at[1 - core], peer_acts, (pair_sems.at[0], pair_sems.at[1]), pair_dev
    )
    acts_copy.start()

    grad_copies = []
    for i, g in enumerate(grad_order):
        load_grads[i].wait()
        picked = jnp.dot(grad_raw[g], onehot, preferred_element_type=jnp.float32)
        mine[g] = (picked * weight).astype(jnp.bfloat16)
        copy = remote(
            mine.at[g], peer.at[g],
            (pair_sems.at[2 + 2 * i], pair_sems.at[3 + 2 * i]), pair_dev,
        )
        copy.start()
        grad_copies.append(copy)
    acts_copy.wait_recv()
    for copy in grad_copies:
        copy.wait_recv()

    def contract(left, right):
        return lax.dot_general(
            left, right, (((1,), (1,)), ((), ())), preferred_element_type=jnp.float32
        )

    def term(step, a, b):
        row = target(step) * 2 + b * (1 - core) + a * core
        column = a * (1 - core) + b * core
        return contract(acts[core, row], mine[column]) + contract(
            peer_acts[row], peer[column]
        )

    def copy_a(step, k):
        return remote(
            send_a.at[step, k], recv_a.at[step, k],
            (a_sems.at[0, step, k], a_sems.at[1, step, k]), a_dev,
        )

    def copy_b(step):
        return remote(
            send_b.at[step], recv_b.at[step],
            (b_sems.at[0, step], b_sems.at[1, step]), b_dev,
        )

    def copy_z(step):
        return remote(
            send_z.at[step], recv_z.at[step],
            (z_sems.at[0, step], z_sems.at[1, step]), z_dev(step),
        )

    def first(step, carry):
        for k in range(2):
            b = 1 - my_b if k == 0 else my_b
            send_a[step, k] = term(step, 1 - my_a, b).astype(jnp.bfloat16)
            copy_a(step, k).start()
        return carry

    def second(step):
        total = term(step, my_a, 1 - my_b)
        copy_a(step, 0).wait_recv()
        total = total + recv_a[step, 0].astype(jnp.float32)
        send_b[step] = total.astype(jnp.bfloat16)
        copy_b(step).start()

    def third(step):
        total = term(step, my_a, my_b)
        copy_a(step, 1).wait_recv()
        total = total + recv_a[step, 1].astype(jnp.float32)
        copy_b(step).wait_recv()
        return total + recv_b[step].astype(jnp.float32)

    def later(step, carry):
        second(step)
        send_z[step - 1] = third(step - 1).astype(jnp.bfloat16)
        copy_z(step - 1).start()
        return carry

    lax.fori_loop(0, outer, first, 0)
    second(0)
    lax.fori_loop(1, outer, later, 0)
    out_ref[...] = third(outer - 1)

    def add(step, carry):
        copy_z(step).wait_recv()
        out_ref[...] += recv_z[step].astype(jnp.float32)
        return carry

    lax.fori_loop(0, outer - 1, add, 0)

    def drain(step, carry):
        copy_a(step, 0).wait_send()
        copy_a(step, 1).wait_send()
        copy_b(step).wait_send()
        return carry

    lax.fori_loop(0, outer, drain, 0)

    def drain_z(step, carry):
        copy_z(step).wait_send()
        return carry

    lax.fori_loop(0, outer - 1, drain_z, 0)
    acts_copy.wait_send()
    for copy in grad_copies:
        copy.wait_send()


def shards(expert_act, grad_out, slot_token, slot_prob, live_count):
    slots, hidden = expert_act.shape
    tokens = grad_out.shape[0]
    ranks, halves = lax.axis_size("dp"), lax.axis_size("tensor")
    outer = ranks // 4
    rows, columns = hidden // ranks, grad_out.shape[1] // halves
    scaling = 1.0 / math.sqrt(slots * ranks * halves)
    bf16, dma = jnp.bfloat16, pltpu.SemaphoreType.DMA
    total = pl.pallas_call(
        functools.partial(kernel, outer),
        out_shape=jax.ShapeDtypeStruct((rows, columns), jnp.float32),
        in_specs=[
            pl.BlockSpec(memory_space=pl.ANY),
            pl.BlockSpec(memory_space=pl.ANY),
            pl.BlockSpec(memory_space=pltpu.VMEM),
            pl.BlockSpec(memory_space=pltpu.VMEM),
            pl.BlockSpec(memory_space=pltpu.SMEM),
        ],
        out_specs=pl.BlockSpec(memory_space=pltpu.VMEM),
        scratch_shapes=[
            pltpu.VMEM((hidden, slots), bf16),
            pltpu.VMEM((halves, columns, tokens), bf16),
            pltpu.VMEM((2, outer * 2, rows, slots), bf16),
            pltpu.VMEM((outer * 2, rows, slots), bf16),
            pltpu.VMEM((halves, columns, slots), bf16),
            pltpu.VMEM((halves, columns, slots), bf16),
            pltpu.VMEM((outer, 2, rows, columns), bf16),
            pltpu.VMEM((outer, 2, rows, columns), bf16),
            pltpu.VMEM((outer, rows, columns), bf16),
            pltpu.VMEM((outer, rows, columns), bf16),
            pltpu.VMEM((outer - 1, rows, columns), bf16),
            pltpu.VMEM((outer - 1, rows, columns), bf16),
            dma((3,)),
            dma((6,)),
            dma((2, outer, 2)),
            dma((2, outer)),
            dma((2, outer - 1)),
        ],
        compiler_params=pltpu.CompilerParams(
            collective_id=0, has_side_effects=True, vmem_limit_bytes=60 * 2**20
        ),
    )(
        expert_act.T,
        grad_out.T.reshape(halves, columns, tokens),
        slot_token[None, :],
        slot_prob[None, :],
        live_count,
    )
    return total * scaling


def solution(mesh):
    return jax.shard_map(
        shards,
        mesh=mesh,
        in_specs=(
            P(("dp", "tensor"), None),
            P(("dp", "tensor"), None),
            P(("dp", "tensor")),
            P(("dp", "tensor")),
            P(("dp", "tensor")),
        ),
        out_specs=P("dp", "tensor"),
        check_vma=False,
    )
```

```python
import functools
import math

import jax
import jax.numpy as jnp
from jax import lax
from jax.experimental import pallas as pl
from jax.experimental.pallas import tpu as pltpu
from jax.sharding import PartitionSpec as P

MESH = pl.DeviceIdType.MESH


def kernel(
    outer,
    acts_hbm, grad_hbm, token_ref, prob_ref, live_ref, out_ref,
    acts_raw, grad_raw, acts, peer_acts, mine, peer,
    send_a, recv_a, send_b, recv_b, send_z, recv_z,
    load_sems, pair_sems, a_sems, b_sems, z_sems,
):
    dp = lax.axis_index("dp")
    half = lax.axis_index("tensor")
    core = lax.rem(dp, 2)
    mid = lax.rem(dp // 2, 2)
    own = dp // 4
    my_a = half * (1 - core) + mid * core
    my_b = mid * (1 - core) + half * core
    flip_mid = dp + 2 - 4 * mid
    pair_dev = {"dp": dp + 1 - 2 * core, "tensor": half}
    a_dev = {
        "dp": dp * (1 - core) + flip_mid * core,
        "tensor": (1 - half) * (1 - core) + half * core,
    }
    b_dev = {
        "dp": flip_mid * (1 - core) + dp * core,
        "tensor": half * (1 - core) + (1 - half) * core,
    }

    def z_dev(step):
        return {"dp": dp + (target(step) - own) * 4, "tensor": half}

    def target(step):
        return lax.rem(own + 1 + step, outer)

    def remote(src, dst, sems, device):
        return pltpu.make_async_remote_copy(
            src_ref=src, dst_ref=dst, send_sem=sems[0], recv_sem=sems[1],
            device_id=device, device_id_type=MESH,
        )

    grad_order = (1 - half, half)
    load_grads = [
        pltpu.make_async_copy(grad_hbm.at[g], grad_raw.at[g], load_sems.at[outer + i])
        for i, g in enumerate(grad_order)
    ]

    def load_acts(step):
        o = target(step)
        return pltpu.make_async_copy(acts_hbm.at[o], acts_raw.at[o], load_sems.at[step])

    load_grads[0].start()
    load_acts(0).start()
    load_grads[1].start()
    for step in range(1, outer):
        load_acts(step).start()

    barrier = pltpu.get_barrier_semaphore()
    for device in [pair_dev, a_dev, b_dev] + [z_dev(s) for s in range(outer - 1)]:
        pl.semaphore_signal(barrier, inc=1, device_id=device, device_id_type=MESH)

    slots, tokens = token_ref.shape[1], grad_raw.shape[2]
    chosen = lax.broadcasted_iota(jnp.int32, (tokens, slots), 0) == token_ref[...]
    onehot = jnp.where(chosen, 1.0, 0.0).astype(jnp.bfloat16)
    live = lax.broadcasted_iota(jnp.int32, (1, slots), 1) < live_ref[0]
    weight = jnp.where(live, prob_ref[...], 0.0)
    rows = acts.shape[3]

    def copy_grad(i):
        g = grad_order[i]
        return remote(
            mine.at[g], peer.at[g],
            (pair_sems.at[0, outer + i], pair_sems.at[1, outer + i]), pair_dev,
        )

    def copy_acts(step):
        o = target(step)
        return remote(
            acts.at[1 - core, o], peer_acts.at[o],
            (pair_sems.at[0, step], pair_sems.at[1, step]), pair_dev,
        )

    def weigh(i):
        g = grad_order[i]
        load_grads[i].wait()
        picked = jnp.dot(grad_raw[g], onehot, preferred_element_type=jnp.float32)
        mine[g] = (picked * weight).astype(jnp.bfloat16)

    def divide(step):
        o = target(step)
        load_acts(step).wait()
        for k in range(4):
            acts[k % 2, o, k // 2] = acts_raw[o, k * rows : (k + 1) * rows, :]

    weigh(0)
    pl.semaphore_wait(barrier, outer + 2)
    copy_grad(0).start()
    divide(0)
    copy_acts(0).start()
    weigh(1)
    copy_grad(1).start()

    def feed(step, carry):
        divide(step)
        copy_acts(step).start()
        return carry

    lax.fori_loop(1, outer, feed, 0)
    copy_grad(0).wait_recv()

    def contract(left, right):
        return lax.dot_general(
            left, right, (((1,), (1,)), ((), ())), preferred_element_type=jnp.float32
        )

    def term(step, a, b):
        o, m = target(step), b * (1 - core) + a * core
        column = a * (1 - core) + b * core
        return contract(acts[core, o, m], mine[column]) + contract(
            peer_acts[o, m], peer[column]
        )

    def copy_a(step, k):
        return remote(
            send_a.at[step, k], recv_a.at[step, k],
            (a_sems.at[0, step, k], a_sems.at[1, step, k]), a_dev,
        )

    def copy_b(step):
        return remote(
            send_b.at[step], recv_b.at[step],
            (b_sems.at[0, step], b_sems.at[1, step]), b_dev,
        )

    def copy_z(step):
        return remote(
            send_z.at[step], recv_z.at[step],
            (z_sems.at[0, step], z_sems.at[1, step]), z_dev(step),
        )

    def first(step, k):
        b = 1 - my_b if k == 0 else my_b
        send_a[step, k] = term(step, 1 - my_a, b).astype(jnp.bfloat16)
        copy_a(step, k).start()

    def second(step):
        total = term(step, my_a, 1 - my_b)
        copy_a(step, 0).wait_recv()
        total = total + recv_a[step, 0].astype(jnp.float32)
        send_b[step] = total.astype(jnp.bfloat16)
        copy_b(step).start()

    def third(step):
        total = term(step, my_a, my_b)
        copy_a(step, 1).wait_recv()
        total = total + recv_a[step, 1].astype(jnp.float32)
        copy_b(step).wait_recv()
        total = total + recv_b[step].astype(jnp.float32)
        send_z[step] = total.astype(jnp.bfloat16)
        copy_z(step).start()

    def stage(step, carry):
        @pl.when(step < outer)
        def _():
            copy_acts(step).wait_recv()
            first(step, 0)

        @pl.when(step == 1)
        def _():
            copy_grad(1).wait_recv()

        @pl.when((step >= 1) & (step <= outer))
        def _():
            first(step - 1, 1)

        @pl.when(step >= 2)
        def _():
            second(step - 2)

        @pl.when(step >= 3)
        def _():
            third(step - 3)

        return carry

    lax.fori_loop(0, outer + 2, stage, 0)
    last = outer - 1
    out_ref[...] = term(last, my_a, my_b)

    def add(step, carry):
        copy_z(step).wait_recv()
        out_ref[...] += recv_z[step].astype(jnp.float32)
        return carry

    lax.fori_loop(0, last, add, 0)
    copy_a(last, 1).wait_recv()
    out_ref[...] += recv_a[last, 1].astype(jnp.float32)
    copy_b(last).wait_recv()
    out_ref[...] += recv_b[last].astype(jnp.float32)

    def drain(step, carry):
        copy_acts(step).wait_send()
        copy_a(step, 0).wait_send()
        copy_a(step, 1).wait_send()
        copy_b(step).wait_send()
        return carry

    lax.fori_loop(0, outer, drain, 0)

    def drain_z(step, carry):
        copy_z(step).wait_send()
        return carry

    lax.fori_loop(0, outer - 1, drain_z, 0)
    copy_grad(0).wait_send()
    copy_grad(1).wait_send()


def shards(expert_act, grad_out, slot_token, slot_prob, live_count):
    slots, hidden = expert_act.shape
    tokens = grad_out.shape[0]
    ranks, halves = lax.axis_size("dp"), lax.axis_size("tensor")
    outer = ranks // 4
    rows, columns = hidden // ranks, grad_out.shape[1] // halves
    scaling = 1.0 / math.sqrt(slots * ranks * halves)
    bf16, dma = jnp.bfloat16, pltpu.SemaphoreType.DMA
    total = pl.pallas_call(
        functools.partial(kernel, outer),
        out_shape=jax.ShapeDtypeStruct((rows, columns), jnp.float32),
        in_specs=[
            pl.BlockSpec(memory_space=pl.ANY),
            pl.BlockSpec(memory_space=pl.ANY),
            pl.BlockSpec(memory_space=pltpu.VMEM),
            pl.BlockSpec(memory_space=pltpu.VMEM),
            pl.BlockSpec(memory_space=pltpu.SMEM),
        ],
        out_specs=pl.BlockSpec(memory_space=pltpu.VMEM),
        scratch_shapes=[
            pltpu.VMEM((outer, 4 * rows, slots), bf16),
            pltpu.VMEM((halves, columns, tokens), bf16),
            pltpu.VMEM((2, outer, 2, rows, slots), bf16),
            pltpu.VMEM((outer, 2, rows, slots), bf16),
            pltpu.VMEM((halves, columns, slots), bf16),
            pltpu.VMEM((halves, columns, slots), bf16),
            pltpu.VMEM((outer, 2, rows, columns), bf16),
            pltpu.VMEM((outer, 2, rows, columns), bf16),
            pltpu.VMEM((outer, rows, columns), bf16),
            pltpu.VMEM((outer, rows, columns), bf16),
            pltpu.VMEM((outer - 1, rows, columns), bf16),
            pltpu.VMEM((outer - 1, rows, columns), bf16),
            dma((outer + 2,)),
            dma((2, outer + 2)),
            dma((2, outer, 2)),
            dma((2, outer)),
            dma((2, outer - 1)),
        ],
        compiler_params=pltpu.CompilerParams(
            collective_id=0, has_side_effects=True, vmem_limit_bytes=60 * 2**20
        ),
    )(
        expert_act.T.reshape(outer, 4 * rows, slots),
        grad_out.T.reshape(halves, columns, tokens),
        slot_token[None, :],
        slot_prob[None, :],
        live_count,
    )
    return total * scaling


def solution(mesh):
    return jax.shard_map(
        shards,
        mesh=mesh,
        in_specs=(
            P(("dp", "tensor"), None),
            P(("dp", "tensor"), None),
            P(("dp", "tensor")),
            P(("dp", "tensor")),
            P(("dp", "tensor")),
        ),
        out_specs=P("dp", "tensor"),
        check_vma=False,
    )
```

```python
import functools
import math

import jax
import jax.numpy as jnp
from jax import lax
from jax.experimental import pallas as pl
from jax.experimental.pallas import tpu as pltpu
from jax.sharding import PartitionSpec as P

MESH = pl.DeviceIdType.MESH


def kernel(
    outer,
    acts_hbm, grad_hbm, token_ref, prob_ref, live_ref, out_ref,
    acts_raw, grad_raw, acts, peer_acts, mine, peer,
    send_a, recv_a, send_b, recv_b, send_z, recv_z,
    load_sems, pair_sems, a_sems, b_sems, z_sems,
):
    dp = lax.axis_index("dp")
    half = lax.axis_index("tensor")
    core = lax.rem(dp, 2)
    mid = lax.rem(dp // 2, 2)
    own = dp // 4
    my_a = half * (1 - core) + mid * core
    my_b = mid * (1 - core) + half * core
    flip_mid = dp + 2 - 4 * mid
    pair_dev = {"dp": dp + 1 - 2 * core, "tensor": half}
    a_dev = {
        "dp": dp * (1 - core) + flip_mid * core,
        "tensor": (1 - half) * (1 - core) + half * core,
    }
    b_dev = {
        "dp": flip_mid * (1 - core) + dp * core,
        "tensor": half * (1 - core) + (1 - half) * core,
    }

    def z_dev(step):
        return {"dp": dp + (target(step) - own) * 4, "tensor": half}

    def target(step):
        offset = outer // 2 + step // 2 - (step % 2) * step
        return lax.rem(own + offset, outer)

    def remote(src, dst, sems, device):
        return pltpu.make_async_remote_copy(
            src_ref=src, dst_ref=dst, send_sem=sems[0], recv_sem=sems[1],
            device_id=device, device_id_type=MESH,
        )

    grad_order = (1 - half, half)
    load_grads = [
        pltpu.make_async_copy(grad_hbm.at[g], grad_raw.at[g], load_sems.at[outer + i])
        for i, g in enumerate(grad_order)
    ]

    def load_acts(step):
        o = target(step)
        return pltpu.make_async_copy(acts_hbm.at[o], acts_raw.at[o], load_sems.at[step])

    load_grads[0].start()
    load_acts(0).start()

    barrier = pltpu.get_barrier_semaphore()
    for device in [pair_dev, a_dev, b_dev] + [z_dev(s) for s in range(outer - 1)]:
        pl.semaphore_signal(barrier, inc=1, device_id=device, device_id_type=MESH)

    slots, tokens = token_ref.shape[1], grad_raw.shape[2]
    chosen = lax.broadcasted_iota(jnp.int32, (tokens, slots), 0) == token_ref[...]
    onehot = jnp.where(chosen, 1.0, 0.0).astype(jnp.bfloat16)
    live = lax.broadcasted_iota(jnp.int32, (1, slots), 1) < live_ref[0]
    weight = jnp.where(live, prob_ref[...], 0.0)
    rows = acts.shape[3]

    def copy_grad(i):
        g = grad_order[i]
        return remote(
            mine.at[g], peer.at[g],
            (pair_sems.at[0, outer + i], pair_sems.at[1, outer + i]), pair_dev,
        )

    def copy_acts(step):
        o = target(step)
        return remote(
            acts.at[1 - core, o], peer_acts.at[o],
            (pair_sems.at[0, step], pair_sems.at[1, step]), pair_dev,
        )

    def weigh(i):
        g = grad_order[i]
        picked = jnp.dot(grad_raw[g], onehot, preferred_element_type=jnp.float32)
        mine[g] = (picked * weight).astype(jnp.bfloat16)

    def divide(step):
        o = target(step)
        load_acts(step).wait()
        for k in range(4):
            acts[k % 2, o, k // 2] = acts_raw[o, k * rows : (k + 1) * rows, :]

    load_grads[0].wait()
    load_grads[1].start()
    weigh(0)
    for step in range(1, outer):
        load_acts(step).start()
    pl.semaphore_wait(barrier, outer + 2)
    copy_grad(0).start()
    divide(0)
    copy_acts(0).start()
    load_grads[1].wait()
    weigh(1)
    copy_grad(1).start()

    def feed(step, carry):
        divide(step)
        copy_acts(step).start()
        return carry

    lax.fori_loop(1, outer, feed, 0)
    copy_grad(0).wait_recv()

    def contract(left, right):
        return lax.dot_general(
            left, right, (((1,), (1,)), ((), ())), preferred_element_type=jnp.float32
        )

    def term(step, a, b):
        o, m = target(step), b * (1 - core) + a * core
        column = a * (1 - core) + b * core
        return contract(acts[core, o, m], mine[column]) + contract(
            peer_acts[o, m], peer[column]
        )

    def copy_a(step, k):
        return remote(
            send_a.at[step, k], recv_a.at[step, k],
            (a_sems.at[0, step, k], a_sems.at[1, step, k]), a_dev,
        )

    def copy_b(step):
        return remote(
            send_b.at[step], recv_b.at[step],
            (b_sems.at[0, step], b_sems.at[1, step]), b_dev,
        )

    def copy_z(step):
        return remote(
            send_z.at[step], recv_z.at[step],
            (z_sems.at[0, step], z_sems.at[1, step]), z_dev(step),
        )

    def first(step, k):
        b = 1 - my_b if k == 0 else my_b
        send_a[step, k] = term(step, 1 - my_a, b).astype(jnp.bfloat16)
        copy_a(step, k).start()

    def second(step):
        total = term(step, my_a, 1 - my_b)
        copy_a(step, 0).wait_recv()
        total = total + recv_a[step, 0].astype(jnp.float32)
        send_b[step] = total.astype(jnp.bfloat16)
        copy_b(step).start()

    def third(step):
        total = term(step, my_a, my_b)
        copy_a(step, 1).wait_recv()
        total = total + recv_a[step, 1].astype(jnp.float32)
        copy_b(step).wait_recv()
        total = total + recv_b[step].astype(jnp.float32)
        send_z[step] = total.astype(jnp.bfloat16)
        copy_z(step).start()

    def stage(step, carry):
        @pl.when(step < outer)
        def _():
            copy_acts(step).wait_recv()
            first(step, 0)

        @pl.when(step == 1)
        def _():
            copy_grad(1).wait_recv()

        @pl.when((step >= 1) & (step <= outer))
        def _():
            first(step - 1, 1)

        @pl.when(step >= 2)
        def _():
            second(step - 2)

        @pl.when(step >= 3)
        def _():
            third(step - 3)

        return carry

    lax.fori_loop(0, outer + 2, stage, 0)
    last = outer - 1
    out_ref[...] = term(last, my_a, my_b)

    def add(step, carry):
        copy_z(step).wait_recv()
        out_ref[...] += recv_z[step].astype(jnp.float32)
        return carry

    lax.fori_loop(0, last, add, 0)
    copy_a(last, 1).wait_recv()
    out_ref[...] += recv_a[last, 1].astype(jnp.float32)
    copy_b(last).wait_recv()
    out_ref[...] += recv_b[last].astype(jnp.float32)

    def drain(step, carry):
        copy_acts(step).wait_send()
        copy_a(step, 0).wait_send()
        copy_a(step, 1).wait_send()
        copy_b(step).wait_send()
        return carry

    lax.fori_loop(0, outer, drain, 0)

    def drain_z(step, carry):
        copy_z(step).wait_send()
        return carry

    lax.fori_loop(0, outer - 1, drain_z, 0)
    copy_grad(0).wait_send()
    copy_grad(1).wait_send()


def shards(expert_act, grad_out, slot_token, slot_prob, live_count):
    slots, hidden = expert_act.shape
    tokens = grad_out.shape[0]
    ranks, halves = lax.axis_size("dp"), lax.axis_size("tensor")
    outer = ranks // 4
    rows, columns = hidden // ranks, grad_out.shape[1] // halves
    scaling = 1.0 / math.sqrt(slots * ranks * halves)
    bf16, dma = jnp.bfloat16, pltpu.SemaphoreType.DMA
    total = pl.pallas_call(
        functools.partial(kernel, outer),
        out_shape=jax.ShapeDtypeStruct((rows, columns), jnp.float32),
        in_specs=[
            pl.BlockSpec(memory_space=pl.ANY),
            pl.BlockSpec(memory_space=pl.ANY),
            pl.BlockSpec(memory_space=pltpu.VMEM),
            pl.BlockSpec(memory_space=pltpu.VMEM),
            pl.BlockSpec(memory_space=pltpu.SMEM),
        ],
        out_specs=pl.BlockSpec(memory_space=pltpu.VMEM),
        scratch_shapes=[
            pltpu.VMEM((outer, 4 * rows, slots), bf16),
            pltpu.VMEM((halves, columns, tokens), bf16),
            pltpu.VMEM((2, outer, 2, rows, slots), bf16),
            pltpu.VMEM((outer, 2, rows, slots), bf16),
            pltpu.VMEM((halves, columns, slots), bf16),
            pltpu.VMEM((halves, columns, slots), bf16),
            pltpu.VMEM((outer, 2, rows, columns), bf16),
            pltpu.VMEM((outer, 2, rows, columns), bf16),
            pltpu.VMEM((outer, rows, columns), bf16),
            pltpu.VMEM((outer, rows, columns), bf16),
            pltpu.VMEM((outer - 1, rows, columns), bf16),
            pltpu.VMEM((outer - 1, rows, columns), bf16),
            dma((outer + 2,)),
            dma((2, outer + 2)),
            dma((2, outer, 2)),
            dma((2, outer)),
            dma((2, outer - 1)),
        ],
        compiler_params=pltpu.CompilerParams(
            collective_id=0, has_side_effects=True, vmem_limit_bytes=60 * 2**20
        ),
    )(
        expert_act.T.reshape(outer, 4 * rows, slots),
        grad_out.T.reshape(halves, columns, tokens),
        slot_token[None, :],
        slot_prob[None, :],
        live_count,
    )
    return total * scaling


def solution(mesh):
    return jax.shard_map(
        shards,
        mesh=mesh,
        in_specs=(
            P(("dp", "tensor"), None),
            P(("dp", "tensor"), None),
            P(("dp", "tensor")),
            P(("dp", "tensor")),
            P(("dp", "tensor")),
        ),
        out_specs=P("dp", "tensor"),
        check_vma=False,
    )
```

```python
import functools
import math

import jax
import jax.numpy as jnp
from jax import lax
from jax.experimental import pallas as pl
from jax.experimental.pallas import tpu as pltpu
from jax.sharding import PartitionSpec as P

MESH = pl.DeviceIdType.MESH


def kernel(
    outer,
    acts_hbm, grad_hbm, token_ref, prob_ref, live_ref, out_ref,
    acts_raw, grad_raw, acts, peer_acts, mine, peer,
    send_a, recv_a, send_b, recv_b, send_z, recv_z,
    load_sems, pair_sems, a_sems, b_sems, z_sems,
):
    dp = lax.axis_index("dp")
    half = lax.axis_index("tensor")
    core = lax.rem(dp, 2)
    mid = lax.rem(dp // 2, 2)
    own = dp // 4
    my_a = half * (1 - core) + mid * core
    my_b = mid * (1 - core) + half * core
    flip_mid = dp + 2 - 4 * mid
    pair_dev = {"dp": dp + 1 - 2 * core, "tensor": half}
    a_dev = {
        "dp": dp * (1 - core) + flip_mid * core,
        "tensor": (1 - half) * (1 - core) + half * core,
    }
    b_dev = {
        "dp": flip_mid * (1 - core) + dp * core,
        "tensor": half * (1 - core) + (1 - half) * core,
    }

    def z_dev(step):
        return {"dp": dp + (target(step) - own) * 4, "tensor": half}

    def target(step):
        offset = outer // 2 + step // 2 - (step % 2) * step
        return lax.rem(own + offset, outer)

    def remote(src, dst, sems, device):
        return pltpu.make_async_remote_copy(
            src_ref=src, dst_ref=dst, send_sem=sems[0], recv_sem=sems[1],
            device_id=device, device_id_type=MESH,
        )

    grad_order = (1 - half, half)
    load_grads = [
        pltpu.make_async_copy(grad_hbm.at[g], grad_raw.at[g], load_sems.at[outer + i])
        for i, g in enumerate(grad_order)
    ]

    def load_acts(step):
        o = target(step)
        return pltpu.make_async_copy(acts_hbm.at[o], acts_raw.at[o], load_sems.at[step])

    load_grads[0].start()
    load_acts(0).start()

    barrier = pltpu.get_barrier_semaphore()
    for device in [pair_dev, a_dev, b_dev] + [z_dev(s) for s in range(outer - 1)]:
        pl.semaphore_signal(barrier, inc=1, device_id=device, device_id_type=MESH)

    slots, tokens = token_ref.shape[1], grad_raw.shape[2]
    chosen = lax.broadcasted_iota(jnp.int32, (tokens, slots), 0) == token_ref[...]
    onehot = jnp.where(chosen, 1.0, 0.0).astype(jnp.bfloat16)
    live = lax.broadcasted_iota(jnp.int32, (1, slots), 1) < live_ref[0]
    weight = jnp.where(live, prob_ref[...], 0.0)
    rows = acts.shape[3]

    def copy_grad(i):
        g = grad_order[i]
        return remote(
            mine.at[g], peer.at[g],
            (pair_sems.at[0, outer + i], pair_sems.at[1, outer + i]), pair_dev,
        )

    def copy_acts(step):
        o = target(step)
        return remote(
            acts.at[1 - core, o], peer_acts.at[o],
            (pair_sems.at[0, step], pair_sems.at[1, step]), pair_dev,
        )

    def weigh(i):
        g = grad_order[i]
        picked = jnp.dot(grad_raw[g], onehot, preferred_element_type=jnp.float32)
        mine[g] = (picked * weight).astype(jnp.bfloat16)

    def divide(step):
        o = target(step)
        load_acts(step).wait()
        for k in range(4):
            acts[k % 2, o, k // 2] = acts_raw[o, k * rows : (k + 1) * rows, :]

    load_grads[0].wait()
    load_grads[1].start()
    weigh(0)
    for step in range(1, outer):
        load_acts(step).start()
    pl.semaphore_wait(barrier, outer + 2)
    copy_grad(0).start()
    divide(0)
    copy_acts(0).start()
    load_grads[1].wait()
    weigh(1)
    copy_grad(1).start()

    def feed(step, carry):
        divide(step)
        copy_acts(step).start()
        return carry

    lax.fori_loop(1, outer, feed, 0)
    copy_grad(0).wait_recv()

    def contract(left, right):
        return lax.dot_general(
            left, right, (((1,), (1,)), ((), ())), preferred_element_type=jnp.float32
        )

    def term(step, a, b):
        o, m = target(step), b * (1 - core) + a * core
        column = a * (1 - core) + b * core
        return contract(acts[core, o, m], mine[column]) + contract(
            peer_acts[o, m], peer[column]
        )

    def copy_a(step, k):
        return remote(
            send_a.at[step, k], recv_a.at[step, k],
            (a_sems.at[0, step, k], a_sems.at[1, step, k]), a_dev,
        )

    def copy_b(step):
        return remote(
            send_b.at[step], recv_b.at[step],
            (b_sems.at[0, step], b_sems.at[1, step]), b_dev,
        )

    def copy_z(step):
        return remote(
            send_z.at[step], recv_z.at[step],
            (z_sems.at[0, step], z_sems.at[1, step]), z_dev(step),
        )

    def first(step, k):
        b = 1 - my_b if k == 0 else my_b
        send_a[step, k] = term(step, 1 - my_a, b).astype(jnp.bfloat16)
        copy_a(step, k).start()

    def second(step):
        total = term(step, my_a, 1 - my_b)
        copy_a(step, 0).wait_recv()
        total = total + recv_a[step, 0].astype(jnp.float32)
        send_b[step] = total.astype(jnp.bfloat16)
        copy_b(step).start()

    def third(step):
        total = term(step, my_a, my_b)
        copy_a(step, 1).wait_recv()
        total = total + recv_a[step, 1].astype(jnp.float32)
        copy_b(step).wait_recv()
        total = total + recv_b[step].astype(jnp.float32)
        send_z[step] = total.astype(jnp.bfloat16)
        copy_z(step).start()

    def stage(step, carry):
        @pl.when(step < outer)
        def _():
            copy_acts(step).wait_recv()
            first(step, 0)

        @pl.when(step == 1)
        def _():
            copy_grad(1).wait_recv()

        @pl.when((step >= 1) & (step <= outer))
        def _():
            first(step - 1, 1)

        @pl.when(step >= 2)
        def _():
            second(step - 2)

        @pl.when(step >= 3)
        def _():
            third(step - 3)

        return carry

    lax.fori_loop(0, outer + 2, stage, 0)
    last = outer - 1
    out_ref[...] = term(last, my_a, my_b)

    def add(step, carry):
        copy_z(step).wait_recv()
        out_ref[...] += recv_z[step].astype(jnp.float32)
        return carry

    lax.fori_loop(0, last, add, 0)
    copy_a(last, 1).wait_recv()
    out_ref[...] += recv_a[last, 1].astype(jnp.float32)
    copy_b(last).wait_recv()
    out_ref[...] += recv_b[last].astype(jnp.float32)

    def drain(step, carry):
        copy_acts(step).wait_send()
        copy_a(step, 0).wait_send()
        copy_a(step, 1).wait_send()
        copy_b(step).wait_send()
        return carry

    lax.fori_loop(0, outer, drain, 0)

    def drain_z(step, carry):
        copy_z(step).wait_send()
        return carry

    lax.fori_loop(0, outer - 1, drain_z, 0)
    copy_grad(0).wait_send()
    copy_grad(1).wait_send()


def shards(expert_act, grad_out, slot_token, slot_prob, live_count):
    slots, hidden = expert_act.shape
    tokens = grad_out.shape[0]
    ranks, halves = lax.axis_size("dp"), lax.axis_size("tensor")
    outer = ranks // 4
    rows, columns = hidden // ranks, grad_out.shape[1] // halves
    scaling = 1.0 / math.sqrt(slots * ranks * halves)
    bf16, dma = jnp.bfloat16, pltpu.SemaphoreType.DMA
    total = pl.pallas_call(
        functools.partial(kernel, outer),
        out_shape=jax.ShapeDtypeStruct((rows, columns), jnp.float32),
        in_specs=[
            pl.BlockSpec(memory_space=pl.ANY),
            pl.BlockSpec(memory_space=pl.ANY),
            pl.BlockSpec(memory_space=pltpu.VMEM),
            pl.BlockSpec(memory_space=pltpu.VMEM),
            pl.BlockSpec(memory_space=pltpu.SMEM),
        ],
        out_specs=pl.BlockSpec(memory_space=pltpu.VMEM),
        scratch_shapes=[
            pltpu.VMEM((outer, 4 * rows, slots), bf16),
            pltpu.VMEM((halves, columns, tokens), bf16),
            pltpu.VMEM((2, outer, 2, rows, slots), bf16),
            pltpu.VMEM((outer, 2, rows, slots), bf16),
            pltpu.VMEM((halves, columns, slots), bf16),
            pltpu.VMEM((halves, columns, slots), bf16),
            pltpu.VMEM((outer, 2, rows, columns), bf16),
            pltpu.VMEM((outer, 2, rows, columns), bf16),
            pltpu.VMEM((outer, rows, columns), bf16),
            pltpu.VMEM((outer, rows, columns), bf16),
            pltpu.VMEM((outer - 1, rows, columns), bf16),
            pltpu.VMEM((outer - 1, rows, columns), bf16),
            dma((outer + 2,)),
            dma((2, outer + 2)),
            dma((2, outer, 2)),
            dma((2, outer)),
            dma((2, outer - 1)),
        ],
        compiler_params=pltpu.CompilerParams(
            collective_id=0, has_side_effects=True, vmem_limit_bytes=53 * 2**20
        ),
    )(
        expert_act.T.reshape(outer, 4 * rows, slots),
        grad_out.T.reshape(halves, columns, tokens),
        slot_token[None, :],
        slot_prob[None, :],
        live_count,
    )
    return total * scaling


def solution(mesh):
    return jax.shard_map(
        shards,
        mesh=mesh,
        in_specs=(
            P(("dp", "tensor"), None),
            P(("dp", "tensor"), None),
            P(("dp", "tensor")),
            P(("dp", "tensor")),
            P(("dp", "tensor")),
        ),
        out_specs=P("dp", "tensor"),
        check_vma=False,
    )
```
